32 devices in a mesh: fy: 2 (over x), fx: 8 (over z, y), ch: 2 (over core).
Axes of the slice: x: 2, y: 2, z: 4, core: 2. Of those that a mesh axis runs over, the one named last changes fastest.
Arguments:
- image_cube: float32 [64, 512, 416], P('ch', 'fx', 'fy'), may hold values from 0 to 2
- data_grad: bfloat16 [64, 512, 416], P('ch', 'fx', 'fy'), may hold values from -6 to 6
- dual_coeffs: float32 [64, 896, 512], P('ch', 'fx', 'fy'), may hold values from -6 to 6
- reweights: float32 [896, 512], P('fx', 'fy'), may hold values from 1 to 40
Outputs:
- image_next: float32 [64, 512, 416], P('ch', 'fx', 'fy')
- dual_next: float32 [64, 896, 512], P('ch', 'fx', 'fy')
The draws below stay inside these ranges and needn't reach their ends.
All inputs are finite; a program needn't handle non-finite values.
Results may differ from the reference program's by a relative error of at most 0.0003.
Values sent between devices are 32-bit elements; how exact they have to be, the bound alone decides.
No kernel may reach another device: no remote copies, remote signals or barrier semaphores. Data moves between devices by JAX's collectives and lax.ppermute only.
A program may use at most 64 MiB of HBM per device.

```python
import math
import jax
import jax.numpy as jnp
import numpy as np
from jax import lax

CH = 64
LEVELS = 2
TX = 64
TY = 208
INTERSECTION = 48
EX = 112
EY = 256
NX = 512
NY = 416
N_FY = 2
N_FX = 8


def steps_of(own_key, dims, shards, low, top_value):
    def one(position, blocks):
        steps = jax.random.uniform(jax.random.fold_in(jax.random.fold_in(own_key, 6), position), (blocks,), jnp.float32, low / len(shards), top_value / len(shards))
        return jnp.repeat(jnp.exp(steps), dims[position] // blocks).reshape((-1,) + (1,) * (len(dims) - position - 1))

    factor_of = one(*shards[0])
    for cut in shards[1:]:
        factor_of = factor_of * one(*cut)
    return factor_of


def noise(stream_key, dims, width, limit, pieces=(), kind=jnp.bfloat16):
    loudness = steps_of(stream_key, dims, pieces, -0.22, 0.18) if pieces else 1.0
    array = jax.random.normal(stream_key, dims, jnp.float32) * width * loudness
    return jnp.minimum(jnp.maximum(array, -limit), limit).astype(kind)


def setup_inputs(seed: int = 0) -> dict:
    keys = jax.random.split(jax.random.key(seed), 5)
    return {
        "image_cube": jnp.clip(2.0 * jax.random.uniform(keys[0], (CH, NX, NY), jnp.float32) ** steps_of(keys[0], (CH, NX, NY), ((0, 2), (1, 8), (2, 2)), -0.2, 0.2), 0.0, 2.0),
        "data_grad": noise(keys[1], (CH, NX, NY), 1.0, 6.0, ((0, 2), (1, 8), (2, 2))),
        "dual_coeffs": noise(keys[2], (CH, N_FX * EX, N_FY * EY), 1.0, 6.0, ((0, 2), (1, 8), (2, 2)), jnp.float32),
        "reweights": jnp.clip(jnp.exp(math.log(40.0) - 3.6888795 * jax.random.uniform(keys[3], (N_FX * EX, N_FY * EY), jnp.float32) ** steps_of(keys[3], (N_FX * EX, N_FY * EY), ((0, 8), (1, 2)), -0.2, 0.2)), 1.0, 40.0),
    }


LOW_PASS = [-0.00011747678400228192, 0.0006754494059985568, -0.0003917403729959771, -0.00487035299301066, 0.008746094047015655, 0.013981027917015516, -0.04408825393106472, -0.01736930100202211, 0.128747426620186, 0.00047248457399797254, -0.2840155429624281, -0.015829105256023893, 0.5853546836548691, 0.6756307362980128, 0.3128715909144659, 0.05441584224308161]
TAU_STEP = 0.5
LAMBDA_REG = 1.0
EPSILON = 1e-06

def level_matrix(length):
    halved = length // 2
    taps_count = len(LOW_PASS)
    matrix = np.zeros((length, length))
    for out_row in range(halved):
        for tap_index in range(taps_count):
            column = (2 * out_row + tap_index) % length
            matrix[out_row, column] += LOW_PASS[tap_index]
            matrix[halved + out_row, column] += (-1) ** tap_index * LOW_PASS[taps_count - 1 - tap_index]
    return matrix

def analysis(facet_block, levels):
    result = facet_block
    width_x = facet_block.shape[1]
    width_y = facet_block.shape[2]
    for level_step in range(levels):
        matrix_x = jnp.asarray(level_matrix(width_x), dtype=facet_block.dtype)
        matrix_y = jnp.asarray(level_matrix(width_y), dtype=facet_block.dtype)
        corner_part = result[:, :width_x, :width_y]
        corner_part = jnp.einsum('cxy,vy->cxv', corner_part, matrix_y, precision=lax.Precision.HIGHEST)
        corner_part = jnp.einsum('ux,cxv->cuv', matrix_x, corner_part, precision=lax.Precision.HIGHEST)
        result = result.at[:, :width_x, :width_y].set(corner_part)
        width_x = width_x // 2
        width_y = width_y // 2
    return result

def synthesis(coeff_block, levels):
    result = coeff_block
    for level_step in range(levels - 1, -1, -1):
        width_x = coeff_block.shape[1] // 2 ** level_step
        width_y = coeff_block.shape[2] // 2 ** level_step
        matrix_x = jnp.asarray(level_matrix(width_x), dtype=coeff_block.dtype)
        matrix_y = jnp.asarray(level_matrix(width_y), dtype=coeff_block.dtype)
        corner_part = result[:, :width_x, :width_y]
        corner_part = jnp.einsum('ux,cuv->cxv', matrix_x, corner_part, precision=lax.Precision.HIGHEST)
        corner_part = jnp.einsum('cxv,vy->cxy', corner_part, matrix_y, precision=lax.Precision.HIGHEST)
        result = result.at[:, :width_x, :width_y].set(corner_part)
    return result

def cover_weights(total, tile, intersection, count, float_kind):
    positions = jnp.arange(total, dtype=jnp.int32)
    offsets = positions % tile
    owners = positions // tile
    edge = (offsets >= tile - intersection) & (owners < count - 1)
    return jnp.where(edge, 0.5 ** 0.5, 1.0).astype(float_kind)

def reference(image_cube, data_grad, dual_coeffs, reweights):
    float_kind = image_cube.dtype
    weight_map = cover_weights(NX, TX, INTERSECTION, N_FX, float_kind)[:, None] * cover_weights(NY, TY, INTERSECTION, N_FY, float_kind)[None, :]
    facets = N_FX * N_FY
    anchor = jnp.int32(0)

    def add_facet(facet_number, accumulated):
        col_index = (facet_number // N_FY).astype(jnp.int32)
        row_index = (facet_number % N_FY).astype(jnp.int32)
        coeff_block = lax.dynamic_slice(dual_coeffs, (anchor, col_index * EX, row_index * EY), (CH, EX, EY))
        piece = synthesis(coeff_block, LEVELS)
        start = (anchor, col_index * TX, row_index * TY)
        current = lax.dynamic_slice(accumulated, start, (CH, EX, EY))
        return lax.dynamic_update_slice(accumulated, current + piece, start)
    accumulated = jnp.zeros((CH, NX + INTERSECTION, NY + INTERSECTION), float_kind)
    accumulated = lax.fori_loop(0, facets, add_facet, accumulated)
    adjoint = accumulated[:, INTERSECTION:, INTERSECTION:] * weight_map
    image_next = jnp.maximum(image_cube - TAU_STEP * (data_grad.astype(float_kind) + adjoint), 0.0)
    extrap = (2.0 * image_next - image_cube) * weight_map
    padded = jnp.pad(extrap, ((0, 0), (INTERSECTION, 0), (INTERSECTION, 0)))

    def new_facet(facet_number, result):
        col_index = (facet_number // N_FY).astype(jnp.int32)
        row_index = (facet_number % N_FY).astype(jnp.int32)
        window = lax.dynamic_slice(padded, (anchor, col_index * TX, row_index * TY), (CH, EX, EY))
        place = (anchor, col_index * EX, row_index * EY)
        updated = lax.dynamic_slice(dual_coeffs, place, (CH, EX, EY)) + analysis(window, LEVELS)
        squared_sum = lax.optimization_barrier(jnp.sum(updated * updated, axis=0))
        local_weights = lax.dynamic_slice(reweights, (col_index * EX, row_index * EY), (EX, EY))
        factor = jnp.minimum(1.0, LAMBDA_REG * local_weights / jnp.sqrt(squared_sum + EPSILON))
        return lax.dynamic_update_slice(result, updated * factor[None], place)
    dual_next = lax.fori_loop(0, facets, new_facet, jnp.zeros_like(dual_coeffs))
    return (image_next, dual_next)
```

```python
import jax
import jax.numpy as jnp
import numpy as np
from jax import lax
from jax.sharding import PartitionSpec as P

LEVELS = 2


LOW_PASS = [
    -0.00011747678400228192,
    0.0006754494059985568,
    -0.0003917403729959771,
    -0.00487035299301066,
    0.008746094047015655,
    0.013981027917015516,
    -0.04408825393106472,
    -0.01736930100202211,
    0.128747426620186,
    0.00047248457399797254,
    -0.2840155429624281,
    -0.015829105256023893,
    0.5853546836548691,
    0.6756307362980128,
    0.3128715909144659,
    0.05441584224308161,
]
TAU_STEP = 0.5
LAMBDA_REG = 1.0
EPSILON = 1e-06


def passed_along(array, axis, by):
    length = lax.axis_size(axis)
    pairs = [(i, i + by) for i in range(length) if 0 <= i + by < length]
    return lax.ppermute(array, axis, pairs)


def level_matrix(length):
    halved = length // 2
    taps_count = len(LOW_PASS)
    matrix = np.zeros((length, length))
    for out_row in range(halved):
        for tap_index in range(taps_count):
            column = (2 * out_row + tap_index) % length
            matrix[out_row, column] += LOW_PASS[tap_index]
            matrix[halved + out_row, column] += (-1) ** tap_index * LOW_PASS[
                taps_count - 1 - tap_index
            ]
    return matrix


def level_einsum(spec, first, second):
    return jnp.einsum(spec, first, second, precision=lax.Precision.HIGH)


def analysis(facet_block, levels):
    result = facet_block
    width_x = facet_block.shape[1]
    width_y = facet_block.shape[2]
    for _ in range(levels):
        matrix_x = jnp.asarray(level_matrix(width_x), dtype=jnp.float32)
        matrix_y = jnp.asarray(level_matrix(width_y), dtype=jnp.float32)
        corner_part = result[:, :width_x, :width_y]
        corner_part = level_einsum("cxy,vy->cxv", corner_part, matrix_y)
        corner_part = level_einsum("ux,cxv->cuv", matrix_x, corner_part)
        result = result.at[:, :width_x, :width_y].set(corner_part)
        width_x = width_x // 2
        width_y = width_y // 2
    return result


def synthesis(coeff_block, levels):
    result = coeff_block
    for level_step in range(levels - 1, -1, -1):
        width_x = coeff_block.shape[1] // 2**level_step
        width_y = coeff_block.shape[2] // 2**level_step
        matrix_x = jnp.asarray(level_matrix(width_x), dtype=jnp.float32)
        matrix_y = jnp.asarray(level_matrix(width_y), dtype=jnp.float32)
        corner_part = result[:, :width_x, :width_y]
        corner_part = level_einsum("ux,cuv->cxv", matrix_x, corner_part)
        corner_part = level_einsum("cxv,vy->cxy", corner_part, matrix_y)
        result = result.at[:, :width_x, :width_y].set(corner_part)
    return result


def tile_weights(length, intersection, position_index, count):
    positions = jnp.arange(length, dtype=jnp.int32)
    edge = (positions >= length - intersection) & (position_index < count - 1)
    return jnp.where(edge, 0.5**0.5, 1.0).astype(jnp.float32)


def group_count(columns, rows):
    best = 1
    for groups in range(1, columns + 1):
        if columns % groups == 0 and (columns // groups) % 8 == 0:
            if padded_size(columns, rows, groups) < padded_size(columns, rows, best):
                best = groups
    return best


def padded_size(columns, rows, groups):
    return (columns // groups) * (-(-(rows * groups) // 128))


def pack(part):
    columns, rows = part.shape[1], part.shape[2]
    groups = group_count(columns, rows)
    step = columns // groups
    return jnp.concatenate([part[:, g * step : (g + 1) * step] for g in range(groups)], axis=2)


def unpack(packed, columns, rows):
    groups = group_count(columns, rows)
    return jnp.concatenate([packed[:, :, g * rows : (g + 1) * rows] for g in range(groups)], axis=1)


def shards(image_cube, data_grad, dual_coeffs, reweights):
    tile_x = image_cube.shape[1]
    tile_y = image_cube.shape[2]
    border = dual_coeffs.shape[1] - tile_x
    head = (tile_y - border) // 128 * 128
    tail = tile_y - head
    weight_map = (
        tile_weights(tile_x, border, lax.axis_index("fx"), lax.axis_size("fx"))[:, None]
        * tile_weights(tile_y, border, lax.axis_index("fy"), lax.axis_size("fy"))[None, :]
    )
    synthesized = synthesis(dual_coeffs, LEVELS)
    upper = jnp.swapaxes(synthesized[:, :, :border], 1, 2)
    from_below = passed_along(upper, "fy", -1)
    own_head = synthesized[:, :, border : border + head]
    from_right_head = passed_along(own_head[:, :border], "fx", -1)
    own_tail = synthesized[:, :, border + head :]
    from_below = jnp.swapaxes(from_below, 1, 2)
    own_tail = own_tail + jnp.pad(from_below, ((0, 0), (0, 0), (tail - border, 0)))
    from_right_tail = unpack(passed_along(pack(own_tail[:, :border]), "fx", -1), border, tail)

    def step(own, incoming, lo, hi):
        summed = own[:, border:] + jnp.pad(incoming, ((0, 0), (tile_x - border, 0), (0, 0)))
        weights = weight_map[:, lo:hi]
        cube = image_cube[:, :, lo:hi]
        grad = data_grad[:, :, lo:hi].astype(jnp.float32)
        image = jnp.maximum(cube - TAU_STEP * (grad + summed * weights), 0.0)
        return image, (2.0 * image - cube) * weights

    image_head, extrap_head = step(own_head, from_right_head, 0, head)
    image_tail, extrap_tail = step(own_tail, from_right_tail, head, tile_y)
    left_tail = unpack(passed_along(pack(extrap_tail[:, tile_x - border :]), "fx", 1), border, tail)
    left_head = passed_along(extrap_head[:, tile_x - border :], "fx", 1)
    rows_tail = jnp.concatenate([left_tail, extrap_tail], axis=1)
    lower = jnp.swapaxes(rows_tail[:, :, tail - border :], 1, 2)
    from_above = jnp.swapaxes(passed_along(lower, "fy", 1), 1, 2)
    rows_head = jnp.concatenate([left_head, extrap_head], axis=1)
    extended = jnp.concatenate([from_above, rows_head, rows_tail], axis=2)
    updated = dual_coeffs + analysis(extended, LEVELS)
    squared_sum = jnp.sum(updated * updated, axis=0)
    pairs = [(i, i ^ 1) for i in range(lax.axis_size("ch"))]
    totals = squared_sum + lax.ppermute(squared_sum, "ch", pairs)
    factor = jnp.minimum(1.0, LAMBDA_REG * reweights / jnp.sqrt(totals + EPSILON))
    image_next = jnp.concatenate([image_head, image_tail], axis=2)
    return (image_next, updated * factor[None])


def solution(mesh):
    return jax.shard_map(
        shards,
        mesh=mesh,
        in_specs=(P("ch", "fx", "fy"), P("ch", "fx", "fy"), P("ch", "fx", "fy"), P("fx", "fy")),
        out_specs=(P("ch", "fx", "fy"), P("ch", "fx", "fy")),
        check_vma=False,
    )
```

```python
import jax
import jax.numpy as jnp
import numpy as np
from jax import lax
from jax.sharding import PartitionSpec as P

LEVELS = 2
CHUNKS = 2


LOW_PASS = [
    -0.00011747678400228192,
    0.0006754494059985568,
    -0.0003917403729959771,
    -0.00487035299301066,
    0.008746094047015655,
    0.013981027917015516,
    -0.04408825393106472,
    -0.01736930100202211,
    0.128747426620186,
    0.00047248457399797254,
    -0.2840155429624281,
    -0.015829105256023893,
    0.5853546836548691,
    0.6756307362980128,
    0.3128715909144659,
    0.05441584224308161,
]
TAU_STEP = 0.5
LAMBDA_REG = 1.0
EPSILON = 1e-06


def passed_along(array, axis, by):
    length = lax.axis_size(axis)
    pairs = [(i, i + by) for i in range(length) if 0 <= i + by < length]
    return lax.ppermute(array, axis, pairs)


def level_matrix(length):
    halved = length // 2
    taps_count = len(LOW_PASS)
    matrix = np.zeros((length, length))
    for out_row in range(halved):
        for tap_index in range(taps_count):
            column = (2 * out_row + tap_index) % length
            matrix[out_row, column] += LOW_PASS[tap_index]
            matrix[halved + out_row, column] += (-1) ** tap_index * LOW_PASS[
                taps_count - 1 - tap_index
            ]
    return matrix


def level_einsum(spec, first, second):
    return jnp.einsum(spec, first, second, precision=lax.Precision.HIGH)


def analysis(facet_block, levels):
    result = facet_block
    width_x = facet_block.shape[1]
    width_y = facet_block.shape[2]
    for _ in range(levels):
        matrix_x = jnp.asarray(level_matrix(width_x), dtype=jnp.float32)
        matrix_y = jnp.asarray(level_matrix(width_y), dtype=jnp.float32)
        corner_part = result[:, :width_x, :width_y]
        corner_part = level_einsum("cxy,vy->cxv", corner_part, matrix_y)
        corner_part = level_einsum("ux,cxv->cuv", matrix_x, corner_part)
        result = result.at[:, :width_x, :width_y].set(corner_part)
        width_x = width_x // 2
        width_y = width_y // 2
    return result


def synthesis(coeff_block, levels):
    result = coeff_block
    for level_step in range(levels - 1, -1, -1):
        width_x = coeff_block.shape[1] // 2**level_step
        width_y = coeff_block.shape[2] // 2**level_step
        matrix_x = jnp.asarray(level_matrix(width_x), dtype=jnp.float32)
        matrix_y = jnp.asarray(level_matrix(width_y), dtype=jnp.float32)
        corner_part = result[:, :width_x, :width_y]
        corner_part = level_einsum("ux,cuv->cxv", matrix_x, corner_part)
        corner_part = level_einsum("cxv,vy->cxy", corner_part, matrix_y)
        result = result.at[:, :width_x, :width_y].set(corner_part)
    return result


def tile_weights(length, intersection, position_index, count):
    positions = jnp.arange(length, dtype=jnp.int32)
    edge = (positions >= length - intersection) & (position_index < count - 1)
    return jnp.where(edge, 0.5**0.5, 1.0).astype(jnp.float32)


def group_count(columns, rows):
    best = 1
    for groups in range(1, columns + 1):
        if columns % groups == 0 and (columns // groups) % 8 == 0:
            if padded_size(columns, rows, groups) < padded_size(columns, rows, best):
                best = groups
    return best


def padded_size(columns, rows, groups):
    return (columns // groups) * (-(-(rows * groups) // 128))


def pack(part):
    columns, rows = part.shape[1], part.shape[2]
    groups = group_count(columns, rows)
    step = columns // groups
    return jnp.concatenate([part[:, g * step : (g + 1) * step] for g in range(groups)], axis=2)


def unpack(packed, columns, rows):
    groups = group_count(columns, rows)
    return jnp.concatenate([packed[:, :, g * rows : (g + 1) * rows] for g in range(groups)], axis=1)


def shards(image_cube, data_grad, dual_coeffs, reweights):
    channels = image_cube.shape[0]
    tile_x = image_cube.shape[1]
    tile_y = image_cube.shape[2]
    border = dual_coeffs.shape[1] - tile_x
    head = (tile_y - border) // 128 * 128
    tail = tile_y - head
    weight_map = (
        tile_weights(tile_x, border, lax.axis_index("fx"), lax.axis_size("fx"))[:, None]
        * tile_weights(tile_y, border, lax.axis_index("fy"), lax.axis_size("fy"))[None, :]
    )
    group = channels // CHUNKS

    def step(own, incoming, held, chunk, lo, hi):
        summed = own[:, border:] + jnp.pad(incoming, ((0, 0), (tile_x - border, 0), (0, 0)))
        weights = held[2][:, lo:hi]
        cube = held[0][chunk, :, lo:hi]
        grad = held[1][chunk, :, lo:hi].astype(jnp.float32)
        image = jnp.maximum(cube - TAU_STEP * (grad + summed * weights), 0.0)
        return image, (2.0 * image - cube) * weights

    images = []
    updates = []
    for n in range(CHUNKS):
        chunk = slice(n * group, (n + 1) * group)
        held = lax.optimization_barrier((image_cube, data_grad, weight_map, dual_coeffs))
        synthesized = synthesis(held[3][chunk], LEVELS)
        own_head = synthesized[:, :, border : border + head]
        from_right_head = passed_along(own_head[:, :border], "fx", -1)
        upper = jnp.swapaxes(synthesized[:, :, :border], 1, 2)
        from_below = jnp.swapaxes(passed_along(upper, "fy", -1), 1, 2)
        own_tail = synthesized[:, :, border + head :]
        own_tail = own_tail + jnp.pad(from_below, ((0, 0), (0, 0), (tail - border, 0)))
        packed = passed_along(pack(own_tail[:, :border]), "fx", -1)
        from_right_tail = unpack(packed, border, tail)
        image_head, extrap_head = step(own_head, from_right_head, held, chunk, 0, head)
        image_tail, extrap_tail = step(own_tail, from_right_tail, held, chunk, head, tile_y)
        packed = passed_along(pack(extrap_tail[:, tile_x - border :]), "fx", 1)
        left_tail = unpack(packed, border, tail)
        left_head = passed_along(extrap_head[:, tile_x - border :], "fx", 1)
        rows_tail = jnp.concatenate([left_tail, extrap_tail], axis=1)
        lower = jnp.swapaxes(rows_tail[:, :, tail - border :], 1, 2)
        from_above = jnp.swapaxes(passed_along(lower, "fy", 1), 1, 2)
        rows_head = jnp.concatenate([left_head, extrap_head], axis=1)
        extended = jnp.concatenate([from_above, rows_head, rows_tail], axis=2)
        updates.append(analysis(extended, LEVELS))
        images.append(jnp.concatenate([image_head, image_tail], axis=2))
    updated = dual_coeffs + jnp.concatenate(updates, axis=0)
    squared_sum = jnp.sum(updated * updated, axis=0)
    pairs = [(i, i ^ 1) for i in range(lax.axis_size("ch"))]
    totals = squared_sum + lax.ppermute(squared_sum, "ch", pairs)
    factor = jnp.minimum(1.0, LAMBDA_REG * reweights / jnp.sqrt(totals + EPSILON))
    return (jnp.concatenate(images, axis=0), updated * factor[None])


def solution(mesh):
    return jax.shard_map(
        shards,
        mesh=mesh,
        in_specs=(P("ch", "fx", "fy"), P("ch", "fx", "fy"), P("ch", "fx", "fy"), P("fx", "fy")),
        out_specs=(P("ch", "fx", "fy"), P("ch", "fx", "fy")),
        check_vma=False,
    )
```

```python
import jax
import jax.numpy as jnp
import numpy as np
from jax import lax
from jax.sharding import PartitionSpec as P

LEVELS = 2


LOW_PASS = [
    -0.00011747678400228192,
    0.0006754494059985568,
    -0.0003917403729959771,
    -0.00487035299301066,
    0.008746094047015655,
    0.013981027917015516,
    -0.04408825393106472,
    -0.01736930100202211,
    0.128747426620186,
    0.00047248457399797254,
    -0.2840155429624281,
    -0.015829105256023893,
    0.5853546836548691,
    0.6756307362980128,
    0.3128715909144659,
    0.05441584224308161,
]
TAU_STEP = 0.5
LAMBDA_REG = 1.0
EPSILON = 1e-06


def passed_along(array, axis, by):
    length = lax.axis_size(axis)
    pairs = [(i, i + by) for i in range(length) if 0 <= i + by < length]
    return lax.ppermute(array, axis, pairs)


def level_matrix(length):
    halved = length // 2
    taps_count = len(LOW_PASS)
    matrix = np.zeros((length, length))
    for out_row in range(halved):
        for tap_index in range(taps_count):
            column = (2 * out_row + tap_index) % length
            matrix[out_row, column] += LOW_PASS[tap_index]
            matrix[halved + out_row, column] += (-1) ** tap_index * LOW_PASS[
                taps_count - 1 - tap_index
            ]
    return matrix


def level_einsum(spec, first, second):
    return jnp.einsum(spec, first, second, precision=lax.Precision.HIGH)


def refine(result, levels):
    width_x = result.shape[1] // 2
    width_y = result.shape[2] // 2
    for _ in range(1, levels):
        matrix_x = jnp.asarray(level_matrix(width_x), dtype=jnp.float32)
        matrix_y = jnp.asarray(level_matrix(width_y), dtype=jnp.float32)
        corner_part = result[:, :width_x, :width_y]
        corner_part = level_einsum("cxy,vy->cxv", corner_part, matrix_y)
        corner_part = level_einsum("ux,cxv->cuv", matrix_x, corner_part)
        result = result.at[:, :width_x, :width_y].set(corner_part)
        width_x = width_x // 2
        width_y = width_y // 2
    return result


def synthesis(coeff_block, levels):
    result = coeff_block
    for level_step in range(levels - 1, -1, -1):
        width_x = coeff_block.shape[1] // 2**level_step
        width_y = coeff_block.shape[2] // 2**level_step
        matrix_x = jnp.asarray(level_matrix(width_x), dtype=jnp.float32)
        matrix_y = jnp.asarray(level_matrix(width_y), dtype=jnp.float32)
        corner_part = result[:, :width_x, :width_y]
        corner_part = level_einsum("ux,cuv->cxv", matrix_x, corner_part)
        corner_part = level_einsum("cxv,vy->cxy", corner_part, matrix_y)
        result = result.at[:, :width_x, :width_y].set(corner_part)
    return result


def tile_weights(length, intersection, position_index, count):
    positions = jnp.arange(length, dtype=jnp.int32)
    edge = (positions >= length - intersection) & (position_index < count - 1)
    return jnp.where(edge, 0.5**0.5, 1.0).astype(jnp.float32)


def group_count(columns, rows):
    best = 1
    for groups in range(1, columns + 1):
        if columns % groups == 0 and (columns // groups) % 8 == 0:
            if padded_size(columns, rows, groups) < padded_size(columns, rows, best):
                best = groups
    return best


def padded_size(columns, rows, groups):
    return (columns // groups) * (-(-(rows * groups) // 128))


def pack(part):
    columns, rows = part.shape[1], part.shape[2]
    groups = group_count(columns, rows)
    step = columns // groups
    return jnp.concatenate([part[:, g * step : (g + 1) * step] for g in range(groups)], axis=2)


def unpack(packed, columns, rows):
    groups = group_count(columns, rows)
    return jnp.concatenate([packed[:, :, g * rows : (g + 1) * rows] for g in range(groups)], axis=1)


def after(array, earlier):
    array, _ = lax.optimization_barrier((array, earlier))
    return array


def sent_packed(part, axis, by):
    columns, rows = part.shape[1], part.shape[2]
    return passed_along(pack(part), axis, by), columns, rows


def shards(image_cube, data_grad, dual_coeffs, reweights):
    tile_x = image_cube.shape[1]
    tile_y = image_cube.shape[2]
    border = dual_coeffs.shape[1] - tile_x
    head = (tile_y - border) // 128 * 128
    tail = tile_y - head
    weight_map = (
        tile_weights(tile_x, border, lax.axis_index("fx"), lax.axis_size("fx"))[:, None]
        * tile_weights(tile_y, border, lax.axis_index("fy"), lax.axis_size("fy"))[None, :]
    )
    synthesized = synthesis(dual_coeffs, LEVELS)
    own_head = synthesized[:, :, border : border + head]
    from_right_head = passed_along(own_head[:, :border], "fx", -1)
    corner = sent_packed(synthesized[:, :border, :border], "fy", -1)
    rest = sent_packed(synthesized[:, border:, :border], "fy", -1)

    def with_rows(own, incoming):
        return own + jnp.pad(incoming, ((0, 0), (0, 0), (tail - border, 0)))

    edge_tail = with_rows(synthesized[:, :border, border + head :], unpack(*corner))
    packed_tail = sent_packed(edge_tail, "fx", -1)

    def step(own, incoming, lo, hi):
        summed = own + jnp.pad(incoming, ((0, 0), (tile_x - border, 0), (0, 0)))
        weights = weight_map[:, lo:hi]
        cube = image_cube[:, :, lo:hi]
        grad = data_grad[:, :, lo:hi].astype(jnp.float32)
        image = jnp.maximum(cube - TAU_STEP * (grad + summed * weights), 0.0)
        return image, (2.0 * image - cube) * weights

    image_head, extrap_head = step(own_head[:, border:], from_right_head, 0, head)
    edge_head = extrap_head[:, tile_x - border :]
    own_tail = with_rows(synthesized[:, border:, border + head :], unpack(*rest))
    from_right_tail = unpack(after(packed_tail[0], (edge_head, own_tail)), border, tail)
    image_tail, extrap_tail = step(own_tail, from_right_tail, head, tile_y)
    packed_tail = sent_packed(extrap_tail[:, tile_x - border :], "fx", 1)
    left_head = passed_along(edge_head, "fx", 1)
    above_own = sent_packed(extrap_tail[:, :, tail - border :], "fy", 1)
    left_tail = unpack(*packed_tail)
    above_corner = sent_packed(left_tail[:, :, tail - border :], "fy", 1)

    matrix_x = jnp.asarray(level_matrix(tile_x + border), dtype=jnp.float32)
    matrix_y = jnp.asarray(level_matrix(tile_y + border), dtype=jnp.float32)
    own = jnp.concatenate([unpack(*above_own), extrap_head, extrap_tail], axis=2)
    own = level_einsum("cxy,vy->cxv", own, matrix_y)
    own = level_einsum("ux,cxv->cuv", matrix_x[:, border:], own)
    image_next = jnp.concatenate([image_head, image_tail], axis=2)
    left_head = after(left_head, (own, image_next))
    edge = jnp.concatenate([unpack(*above_corner), left_head, left_tail], axis=2)
    edge = level_einsum("cxy,vy->cxv", edge, matrix_y)
    edge = level_einsum("ux,cxv->cuv", matrix_x[:, :border], edge)
    updated = dual_coeffs + refine(own + edge, LEVELS)
    squared_sum = jnp.sum(updated * updated, axis=0)
    pairs = [(i, i ^ 1) for i in range(lax.axis_size("ch"))]
    totals = squared_sum + lax.ppermute(squared_sum, "ch", pairs)
    factor = jnp.minimum(1.0, LAMBDA_REG * reweights / jnp.sqrt(totals + EPSILON))
    return (image_next, updated * factor[None])


def solution(mesh):
    return jax.shard_map(
        shards,
        mesh=mesh,
        in_specs=(P("ch", "fx", "fy"), P("ch", "fx", "fy"), P("ch", "fx", "fy"), P("fx", "fy")),
        out_specs=(P("ch", "fx", "fy"), P("ch", "fx", "fy")),
        check_vma=False,
    )
```

```python
import jax
import jax.numpy as jnp
import numpy as np
from jax import lax
from jax.sharding import PartitionSpec as P

LEVELS = 2


LOW_PASS = [
    -0.00011747678400228192,
    0.0006754494059985568,
    -0.0003917403729959771,
    -0.00487035299301066,
    0.008746094047015655,
    0.013981027917015516,
    -0.04408825393106472,
    -0.01736930100202211,
    0.128747426620186,
    0.00047248457399797254,
    -0.2840155429624281,
    -0.015829105256023893,
    0.5853546836548691,
    0.6756307362980128,
    0.3128715909144659,
    0.05441584224308161,
]
TAU_STEP = 0.5
LAMBDA_REG = 1.0
EPSILON = 1e-06


def passed_along(array, axis, by):
    length = lax.axis_size(axis)
    pairs = [(i, i + by) for i in range(length) if 0 <= i + by < length]
    return lax.ppermute(array, axis, pairs)


def level_matrix(length):
    halved = length // 2
    taps_count = len(LOW_PASS)
    matrix = np.zeros((length, length))
    for out_row in range(halved):
        for tap_index in range(taps_count):
            column = (2 * out_row + tap_index) % length
            matrix[out_row, column] += LOW_PASS[tap_index]
            matrix[halved + out_row, column] += (-1) ** tap_index * LOW_PASS[
                taps_count - 1 - tap_index
            ]
    return matrix


def level_einsum(spec, first, second):
    return jnp.einsum(spec, first, second, precision=lax.Precision.HIGH)


def refine(result, levels):
    width_x = result.shape[1] // 2
    width_y = result.shape[2] // 2
    for _ in range(1, levels):
        matrix_x = jnp.asarray(level_matrix(width_x), dtype=jnp.float32)
        matrix_y = jnp.asarray(level_matrix(width_y), dtype=jnp.float32)
        corner_part = result[:, :width_x, :width_y]
        corner_part = level_einsum("cxy,vy->cxv", corner_part, matrix_y)
        corner_part = level_einsum("ux,cxv->cuv", matrix_x, corner_part)
        result = result.at[:, :width_x, :width_y].set(corner_part)
        width_x = width_x // 2
        width_y = width_y // 2
    return result


def synthesis(coeff_block, levels):
    result = coeff_block
    for level_step in range(levels - 1, -1, -1):
        width_x = coeff_block.shape[1] // 2**level_step
        width_y = coeff_block.shape[2] // 2**level_step
        matrix_x = jnp.asarray(level_matrix(width_x), dtype=jnp.float32)
        matrix_y = jnp.asarray(level_matrix(width_y), dtype=jnp.float32)
        corner_part = result[:, :width_x, :width_y]
        corner_part = level_einsum("ux,cuv->cxv", matrix_x, corner_part)
        corner_part = level_einsum("cxv,vy->cxy", corner_part, matrix_y)
        result = result.at[:, :width_x, :width_y].set(corner_part)
    return result


def tile_weights(length, intersection, position_index, count):
    positions = jnp.arange(length, dtype=jnp.int32)
    edge = (positions >= length - intersection) & (position_index < count - 1)
    return jnp.where(edge, 0.5**0.5, 1.0).astype(jnp.float32)


def group_count(columns, rows):
    best = 1
    for groups in range(1, columns + 1):
        if columns % groups == 0 and (columns // groups) % 8 == 0:
            if padded_size(columns, rows, groups) < padded_size(columns, rows, best):
                best = groups
    return best


def padded_size(columns, rows, groups):
    return (columns // groups) * (-(-(rows * groups) // 128))


def pack(part):
    columns, rows = part.shape[1], part.shape[2]
    groups = group_count(columns, rows)
    step = columns // groups
    return jnp.concatenate([part[:, g * step : (g + 1) * step] for g in range(groups)], axis=2)


def unpack(packed, columns, rows):
    groups = group_count(columns, rows)
    return jnp.concatenate([packed[:, :, g * rows : (g + 1) * rows] for g in range(groups)], axis=1)


def after(array, earlier):
    array, _ = lax.optimization_barrier((array, earlier))
    return array


def sent_packed(part, axis, by):
    columns, rows = part.shape[1], part.shape[2]
    return passed_along(pack(part), axis, by), columns, rows


def shards(image_cube, data_grad, dual_coeffs, reweights):
    tile_x = image_cube.shape[1]
    tile_y = image_cube.shape[2]
    border = dual_coeffs.shape[1] - tile_x
    head = (tile_y - border) // 128 * 128
    tail = tile_y - head
    weight_map = (
        tile_weights(tile_x, border, lax.axis_index("fx"), lax.axis_size("fx"))[:, None]
        * tile_weights(tile_y, border, lax.axis_index("fy"), lax.axis_size("fy"))[None, :]
    )
    synthesized = synthesis(dual_coeffs, LEVELS)
    own_head = synthesized[:, :, border : border + head]
    from_right_head = passed_along(own_head[:, :border], "fx", -1)
    corner = sent_packed(synthesized[:, :border, :border], "fy", -1)
    rest = sent_packed(synthesized[:, border:, :border], "fy", -1)

    def with_rows(own, incoming):
        return own + jnp.pad(incoming, ((0, 0), (0, 0), (tail - border, 0)))

    edge_tail = with_rows(synthesized[:, :border, border + head :], unpack(*corner))
    packed_tail = sent_packed(edge_tail, "fx", -1)

    def step(own, incoming, lo, hi):
        summed = own + jnp.pad(incoming, ((0, 0), (tile_x - border, 0), (0, 0)))
        weights = weight_map[:, lo:hi]
        cube = image_cube[:, :, lo:hi]
        grad = data_grad[:, :, lo:hi].astype(jnp.float32)
        image = jnp.maximum(cube - TAU_STEP * (grad + summed * weights), 0.0)
        return image, (2.0 * image - cube) * weights

    image_head, extrap_head = step(own_head[:, border:], from_right_head, 0, head)
    edge_head = extrap_head[:, tile_x - border :]
    half = edge_head.shape[0] // 2
    first_half = passed_along(edge_head[:half], "fx", 1)
    own_tail = with_rows(synthesized[:, border:, border + head :], unpack(*rest))
    from_right_tail = unpack(after(packed_tail[0], (edge_head, own_tail)), border, tail)
    image_tail, extrap_tail = step(own_tail, from_right_tail, head, tile_y)
    edge_tail = pack(extrap_tail[:, tile_x - border :])
    left_tail = unpack(passed_along(edge_tail, "fx", 1), border, tail)
    second_half = passed_along(edge_head[half:], "fx", 1)
    own_rows = after(extrap_tail, edge_tail)[:, :, tail - border :]
    above_own = passed_along(pack(own_rows), "fy", 1)
    edge_corner = pack(left_tail[:, :, tail - border :])
    above_corner = unpack(passed_along(edge_corner, "fy", 1), border, border)
    above_own = unpack(after(above_own, edge_corner), tile_x, border)

    matrix_x = jnp.asarray(level_matrix(tile_x + border), dtype=jnp.float32)
    matrix_y = jnp.asarray(level_matrix(tile_y + border), dtype=jnp.float32)
    own = jnp.concatenate([above_own, extrap_head, extrap_tail], axis=2)
    own = level_einsum("cxy,vy->cxv", own, matrix_y)
    own = level_einsum("ux,cxv->cuv", matrix_x[:, border:], own)
    image_next = jnp.concatenate([image_head, image_tail], axis=2)
    second_half = after(second_half, (own, image_next))
    left_head = jnp.concatenate([first_half, second_half], axis=0)
    edge = jnp.concatenate([above_corner, left_head, left_tail], axis=2)
    edge = level_einsum("cxy,vy->cxv", edge, matrix_y)
    edge = level_einsum("ux,cxv->cuv", matrix_x[:, :border], edge)
    updated = dual_coeffs + refine(own + edge, LEVELS)
    squared_sum = jnp.sum(updated * updated, axis=0)
    pairs = [(i, i ^ 1) for i in range(lax.axis_size("ch"))]
    totals = squared_sum + lax.ppermute(squared_sum, "ch", pairs)
    factor = jnp.minimum(1.0, LAMBDA_REG * reweights / jnp.sqrt(totals + EPSILON))
    return (image_next, updated * factor[None])


def solution(mesh):
    return jax.shard_map(
        shards,
        mesh=mesh,
        in_specs=(P("ch", "fx", "fy"), P("ch", "fx", "fy"), P("ch", "fx", "fy"), P("fx", "fy")),
        out_specs=(P("ch", "fx", "fy"), P("ch", "fx", "fy")),
        check_vma=False,
    )
```

```python
import jax
import jax.numpy as jnp
import numpy as np
from jax import lax
from jax.sharding import PartitionSpec as P

LEVELS = 2


LOW_PASS = [
    -0.00011747678400228192,
    0.0006754494059985568,
    -0.0003917403729959771,
    -0.00487035299301066,
    0.008746094047015655,
    0.013981027917015516,
    -0.04408825393106472,
    -0.01736930100202211,
    0.128747426620186,
    0.00047248457399797254,
    -0.2840155429624281,
    -0.015829105256023893,
    0.5853546836548691,
    0.6756307362980128,
    0.3128715909144659,
    0.05441584224308161,
]
TAU_STEP = 0.5
LAMBDA_REG = 1.0
EPSILON = 1e-06


def passed_along(array, axis, by):
    length = lax.axis_size(axis)
    pairs = [(i, i + by) for i in range(length) if 0 <= i + by < length]
    return lax.ppermute(array, axis, pairs)


def level_matrix(length):
    halved = length // 2
    taps_count = len(LOW_PASS)
    matrix = np.zeros((length, length))
    for out_row in range(halved):
        for tap_index in range(taps_count):
            column = (2 * out_row + tap_index) % length
            matrix[out_row, column] += LOW_PASS[tap_index]
            matrix[halved + out_row, column] += (-1) ** tap_index * LOW_PASS[
                taps_count - 1 - tap_index
            ]
    return matrix


def level_einsum(spec, first, second):
    return jnp.einsum(spec, first, second, precision=lax.Precision.HIGH)


def refine(result, levels):
    width_x = result.shape[1] // 2
    width_y = result.shape[2] // 2
    for _ in range(1, levels):
        matrix_x = jnp.asarray(level_matrix(width_x), dtype=jnp.float32)
        matrix_y = jnp.asarray(level_matrix(width_y), dtype=jnp.float32)
        corner_part = result[:, :width_x, :width_y]
        corner_part = level_einsum("cxy,vy->cxv", corner_part, matrix_y)
        corner_part = level_einsum("ux,cxv->cuv", matrix_x, corner_part)
        result = result.at[:, :width_x, :width_y].set(corner_part)
        width_x = width_x // 2
        width_y = width_y // 2
    return result


def synthesis(coeff_block, levels):
    result = coeff_block
    for level_step in range(levels - 1, -1, -1):
        width_x = coeff_block.shape[1] // 2**level_step
        width_y = coeff_block.shape[2] // 2**level_step
        matrix_x = jnp.asarray(level_matrix(width_x), dtype=jnp.float32)
        matrix_y = jnp.asarray(level_matrix(width_y), dtype=jnp.float32)
        corner_part = result[:, :width_x, :width_y]
        corner_part = level_einsum("ux,cuv->cxv", matrix_x, corner_part)
        corner_part = level_einsum("cxv,vy->cxy", corner_part, matrix_y)
        result = result.at[:, :width_x, :width_y].set(corner_part)
    return result


def tile_weights(length, intersection, position_index, count):
    positions = jnp.arange(length, dtype=jnp.int32)
    edge = (positions >= length - intersection) & (position_index < count - 1)
    return jnp.where(edge, 0.5**0.5, 1.0).astype(jnp.float32)


def group_count(columns, rows):
    best = 1
    for groups in range(1, columns + 1):
        if columns % groups == 0 and (columns // groups) % 8 == 0:
            if padded_size(columns, rows, groups) < padded_size(columns, rows, best):
                best = groups
    return best


def padded_size(columns, rows, groups):
    return (columns // groups) * (-(-(rows * groups) // 128))


def pack(part):
    columns, rows = part.shape[1], part.shape[2]
    groups = group_count(columns, rows)
    step = columns // groups
    return jnp.concatenate([part[:, g * step : (g + 1) * step] for g in range(groups)], axis=2)


def unpack(packed, columns, rows):
    groups = group_count(columns, rows)
    return jnp.concatenate([packed[:, :, g * rows : (g + 1) * rows] for g in range(groups)], axis=1)


def after(array, earlier):
    array, _ = lax.optimization_barrier((array, earlier))
    return array


def sent_packed(part, axis, by):
    columns, rows = part.shape[1], part.shape[2]
    return passed_along(pack(part), axis, by), columns, rows


def shards(image_cube, data_grad, dual_coeffs, reweights):
    tile_x = image_cube.shape[1]
    tile_y = image_cube.shape[2]
    border = dual_coeffs.shape[1] - tile_x
    head = (tile_y - border) // 128 * 128
    tail = tile_y - head
    weight_map = (
        tile_weights(tile_x, border, lax.axis_index("fx"), lax.axis_size("fx"))[:, None]
        * tile_weights(tile_y, border, lax.axis_index("fy"), lax.axis_size("fy"))[None, :]
    )
    synthesized = synthesis(dual_coeffs, LEVELS)
    own_head = synthesized[:, :, border : border + head]
    from_right_head = passed_along(own_head[:, :border], "fx", -1)
    corner = sent_packed(synthesized[:, :border, :border], "fy", -1)
    rest = sent_packed(synthesized[:, border:, :border], "fy", -1)

    def with_rows(own, incoming):
        return own + jnp.pad(incoming, ((0, 0), (0, 0), (tail - border, 0)))

    edge_tail = with_rows(synthesized[:, :border, border + head :], unpack(*corner))
    packed_tail = sent_packed(edge_tail, "fx", -1)

    def step(own, incoming, lo, hi):
        summed = own + jnp.pad(incoming, ((0, 0), (tile_x - border, 0), (0, 0)))
        weights = weight_map[:, lo:hi]
        cube = image_cube[:, :, lo:hi]
        grad = data_grad[:, :, lo:hi].astype(jnp.float32)
        image = jnp.maximum(cube - TAU_STEP * (grad + summed * weights), 0.0)
        return image, (2.0 * image - cube) * weights

    image_head, extrap_head = step(own_head[:, border:], from_right_head, 0, head)
    edge_head = extrap_head[:, tile_x - border :]
    own_tail = with_rows(synthesized[:, border:, border + head :], unpack(*rest))
    from_right_tail = unpack(after(packed_tail[0], (edge_head, own_tail)), border, tail)
    image_tail, extrap_tail = step(own_tail, from_right_tail, head, tile_y)
    edge_tail = pack(extrap_tail[:, tile_x - border :])
    left_tail = unpack(passed_along(edge_tail, "fx", 1), border, tail)
    left_head = passed_along(edge_head, "fx", 1)
    own_rows = after(extrap_tail, edge_tail)[:, :, tail - border :]
    above_own = passed_along(pack(own_rows), "fy", 1)
    edge_corner = pack(left_tail[:, :, tail - border :])
    above_corner = unpack(passed_along(edge_corner, "fy", 1), border, border)
    above_own = unpack(after(above_own, edge_corner), tile_x, border)

    matrix_x = jnp.asarray(level_matrix(tile_x + border), dtype=jnp.float32)
    matrix_y = jnp.asarray(level_matrix(tile_y + border), dtype=jnp.float32)
    own = jnp.concatenate([above_own, extrap_head, extrap_tail], axis=2)
    own = level_einsum("cxy,vy->cxv", own, matrix_y)
    own = level_einsum("ux,cxv->cuv", matrix_x[:, border:], own)
    image_next = jnp.concatenate([image_head, image_tail], axis=2)
    left_head = after(left_head, (own, image_next))
    edge = jnp.concatenate([above_corner, left_head, left_tail], axis=2)
    edge = level_einsum("cxy,vy->cxv", edge, matrix_y)
    edge = level_einsum("ux,cxv->cuv", matrix_x[:, :border], edge)
    updated = dual_coeffs + refine(own + edge, LEVELS)
    squared_sum = jnp.sum(updated * updated, axis=0)
    pairs = [(i, i ^ 1) for i in range(lax.axis_size("ch"))]
    totals = squared_sum + lax.ppermute(squared_sum, "ch", pairs)
    factor = jnp.minimum(1.0, LAMBDA_REG * reweights / jnp.sqrt(totals + EPSILON))
    return (image_next, updated * factor[None])


def solution(mesh):
    return jax.shard_map(
        shards,
        mesh=mesh,
        in_specs=(P("ch", "fx", "fy"), P("ch", "fx", "fy"), P("ch", "fx", "fy"), P("fx", "fy")),
        out_specs=(P("ch", "fx", "fy"), P("ch", "fx", "fy")),
        check_vma=False,
    )
```
